256 devices in a mesh: gx: 8 (over y, z_lo), gy: 8 (over x, core), gz: 4 (over z_hi).
Axes of the slice: x: 4, y: 4, z: 8 (z_hi: 4, z_lo: 2; z = z_hi * 2 + z_lo), core: 2. Of those that a mesh axis runs over, the one named last changes fastest.
Arguments:
- features: bfloat16 [32, 64, 2048], P('gx', 'gy', 'gz'), may hold values from -6 to 6
- upstream: bfloat16 [32, 64, 2048], P('gx', 'gy', 'gz'), may hold values from -6 to 6
- params: float32 [718848], P(('gx', 'gy', 'gz')), may hold values from -1 to 1
- first_moment: float32 [718848], P(('gx', 'gy', 'gz')), may hold values from -1 to 1
- second_moment: float32 [718848], P(('gx', 'gy', 'gz')), may hold values from 0.0005 to 0.005
Outputs:
- refined: bfloat16 [32, 64, 2048], P('gx', 'gy', 'gz')
- new_params: float32 [718848], P(('gx', 'gy', 'gz'))
- new_first: float32 [718848], P(('gx', 'gy', 'gz'))
- new_second: float32 [718848], P(('gx', 'gy', 'gz'))
The draws below stay inside these ranges and needn't reach their ends.
All inputs are finite; a program needn't handle non-finite values.
Results may differ from the reference program's by a relative error of at most 0.01.
The reference program's roundings to bfloat16 on the way count: a program that leaves them out, or rounds other values in their place, can miss the bound.
Values may be sent and summed in bfloat16 or wider, within the bound.
No kernel may reach another device: no remote copies, remote signals or barrier semaphores. Data moves between devices by JAX's collectives and lax.ppermute only.
A program may use at most 128 MiB of HBM per device.

```python
import math
import jax
import jax.numpy as jnp
from jax import lax

C = 64
G = 32
STEP = 3
NX = 32
NY = 64
NZ = 32
PARAMS = 718848


def draw_params(key, part):
    shapes = [(G, C + layer * G) for layer in range(4)] + [(C, C + 4 * G)]
    segments = []
    for layer in range(5):
        outputs, inputs = shapes[layer]
        sub_key = jax.random.fold_in(key, 11 + layer)
        spread = (27.0 * inputs) ** (-0.5)
        values = jnp.clip(jax.random.normal(sub_key, (27 * outputs * inputs,), jnp.float32), -3.0, 3.0) * spread
        segments.append(values)
    return jnp.concatenate(segments)


def level_of(stream_key, extent, cuts, smallest, largest):
    loudness = 1.0
    for axis_at, shards_of in cuts:
        heights = jax.random.uniform(jax.random.fold_in(jax.random.fold_in(stream_key, 6), axis_at), (shards_of,), jnp.float32, smallest / len(cuts), largest / len(cuts))
        loudness = loudness * jnp.repeat(jnp.exp(heights), extent[axis_at] // shards_of).reshape((-1,) + (1,) * (len(extent) - 1 - axis_at))
    return loudness


def centred(rng, shape, deviation, most, shards=(), dtype=jnp.bfloat16):
    loudness = level_of(rng, shape, shards, -0.22, 0.18) if shards else 1.0
    values = jax.random.normal(rng, shape, jnp.float32) * deviation * loudness
    return jnp.minimum(jnp.maximum(values, -most), most).astype(dtype)


def setup_inputs(seed: int = 0) -> dict:
    keys = jax.random.split(jax.random.key(seed), 6)
    return {
        "features": centred(keys[0], (NX, NY, NZ * C), 1.0, 6.0, ((0, 8), (1, 8), (2, 4))),
        "upstream": centred(keys[1], (NX, NY, NZ * C), 1.0, 6.0, ((0, 8), (1, 8), (2, 4))),
        "params": draw_params(jax.random.fold_in(keys[5], 71), 0),
        "first_moment": centred(keys[3], (PARAMS,), 0.2, 1.0, ((0, 256),), jnp.float32),
        "second_moment": jnp.clip(jnp.exp(math.log(0.005) - 2.30258502 * jax.random.uniform(keys[4], (PARAMS,), jnp.float32) ** level_of(keys[4], (PARAMS,), ((0, 256),), -0.2, 0.2)), 0.0005, 0.005),
    }


LEAK_SLOPE = 0.2
RESIDUAL_SCALE = 0.2
BETA_ONE = 0.9
BETA_TWO = 0.999
LEARN_RATE = 0.001
ADAM_EPS = 1e-08
NORM_EPS = 1e-06

def layer_shapes():
    return [(G, C + layer * G) for layer in range(4)] + [(C, C + 4 * G)]

def split_kernels(flat_weights):
    kernel_list = []
    offset = 0
    for outputs, inputs in layer_shapes():
        length = 27 * outputs * inputs
        kernel_list.append(flat_weights[offset:offset + length].reshape(27, outputs, inputs))
        offset = offset + length
    return kernel_list

def correlate(values_in, kernel):
    weight = kernel.astype(jnp.float32).reshape(3, 3, 3, kernel.shape[1], kernel.shape[2]).transpose(3, 4, 0, 1, 2)
    result = lax.conv_general_dilated(values_in.astype(jnp.float32)[None], weight, (1, 1, 1), [(1, 1), (1, 1), (1, 1)], dimension_numbers=('NCDHW', 'OIDHW', 'NCDHW'), precision=lax.Precision.HIGHEST)
    return result[0]

def channels_first(packed):
    return packed.reshape(packed.shape[0], packed.shape[1], -1, C).transpose(3, 0, 1, 2)

def reference(features, upstream, params, first_moment, second_moment):
    field = channels_first(features)
    dout = channels_first(upstream)
    kernel_list = split_kernels(params.astype(jnp.bfloat16))
    pieces = [field]
    slopes = []
    for layer in range(4):
        before = correlate(jnp.concatenate(pieces, 0), kernel_list[layer])
        slope_now = jnp.where(before > 0, 1.0, LEAK_SLOPE).astype(jnp.float32)
        slopes.append(slope_now)
        pieces.append((before * slope_now).astype(jnp.bfloat16))
    inputs_list = [jnp.concatenate(pieces[:layer + 1], 0) for layer in range(5)]
    last = correlate(inputs_list[4], kernel_list[4])
    refined_first = (field.astype(jnp.float32) + RESIDUAL_SCALE * last).astype(jnp.bfloat16)
    refined = refined_first.transpose(1, 2, 3, 0).reshape(features.shape)
    signals = [None] * 5
    signals[4] = (RESIDUAL_SCALE * dout.astype(jnp.float32)).astype(jnp.bfloat16)
    backward = [jnp.zeros((G,) + field.shape[1:], jnp.float32) for layer in range(4)]
    for layer in range(4, 0, -1):
        kernel_now = kernel_list[layer]

        def convolve(values_in):
            return correlate(values_in, kernel_now)
        unused, pullback = jax.vjp(convolve, inputs_list[layer].astype(jnp.float32))
        spread = pullback(signals[layer].astype(jnp.float32))[0]
        for target in range(layer):
            backward[target] = backward[target] + spread[C + target * G:C + (target + 1) * G]
        signals[layer - 1] = (backward[layer - 1] * slopes[layer - 1]).astype(jnp.bfloat16)
    grads = []
    for layer in range(5):
        input_now = inputs_list[layer]

        def convolve_kernel(kernel):
            return correlate(input_now, kernel)
        unused, pullback = jax.vjp(convolve_kernel, kernel_list[layer].astype(jnp.float32))
        grads.append(pullback(signals[layer].astype(jnp.float32))[0].reshape(-1))
    gradient = jnp.concatenate(grads)
    norm_sq = jnp.sum(gradient * gradient)
    factor = jnp.minimum(1.0, jnp.sqrt(PARAMS / (norm_sq + NORM_EPS)))
    clipped = gradient * factor
    new_first = BETA_ONE * first_moment + (1.0 - BETA_ONE) * clipped
    new_second = BETA_TWO * second_moment + (1.0 - BETA_TWO) * clipped * clipped
    first_hat = new_first / (1.0 - BETA_ONE ** STEP)
    second_hat = new_second / (1.0 - BETA_TWO ** STEP)
    new_params = params - LEARN_RATE * first_hat / (jnp.sqrt(second_hat) + ADAM_EPS)
    return (refined, new_params, new_first, new_second)
```

```python
import functools

import jax
import jax.numpy as jnp
from jax import lax
from jax.experimental import pallas as pl
from jax.experimental.pallas import tpu as pltpu
from jax.sharding import PartitionSpec as P

C = 64
G = 32
STEP = 3
AXES = ("gx", "gy", "gz")

LEAK_SLOPE = 0.2
RESIDUAL_SCALE = 0.2
BETA_ONE = 0.9
BETA_TWO = 0.999
LEARN_RATE = 0.001
ADAM_EPS = 1e-08
NORM_EPS = 1e-06

SIZE_X, SIZE_Y, SIZE_Z = 4, 8, 8
HALO = 4
FULL = (SIZE_X + 2 * HALO, SIZE_Y + 2 * HALO, SIZE_Z + 2 * HALO)
EXTENTS = (3, 2, 1, 0)
NARROW = 3
INPUTS = [C + layer * G for layer in range(5)]
OUTPUTS = [G] * 4 + [C]
BF16 = jnp.bfloat16
F32 = jnp.float32
NT = (((1,), (1,)), ((), ()))
NN = (((1,), (0,)), ((), ()))


def swap_sides(cells, axis, dim, width):
    count = lax.axis_size(axis)
    size = cells.shape[dim]
    tail = lax.slice_in_dim(cells, size - width, size, axis=dim)
    head = lax.slice_in_dim(cells, 0, width, axis=dim)
    below = lax.ppermute(tail, axis, [(i, i + 1) for i in range(count - 1)])
    above = lax.ppermute(head, axis, [(i + 1, i) for i in range(count - 1)])
    return jnp.concatenate([below, cells, above], axis=dim)


def exchange_stages():
    nx, ny, nz = (lax.axis_size(name) for name in AXES)
    stages = [
        [r for r in range(1, nz)],
        [2 * r * ny * nz for r in range(1, nx // 2)],
        [ny * nz],
        [2 * r * nz for r in range(1, ny // 2)],
        [nz],
    ]
    return [stage for stage in stages if stage]


def send_to(cells, mask):
    devices = lax.axis_size(AXES)
    return lax.ppermute(cells, AXES, [(i, i ^ mask) for i in range(devices)])


def place_of(x, y, z, nx, ny, nz):
    return z + nz * ((x >> 1) + (nx // 2) * ((x & 1) + 2 * ((y >> 1) + (ny // 2) * (y & 1))))


def places(nx, ny, nz):
    return [place_of(d // (ny * nz), d // nz % ny, d % nz, nx, ny, nz) for d in range(nx * ny * nz)]


def gather_blocks(block):
    block = block[None]
    for stage in exchange_stages():
        block = jnp.concatenate([block] + [send_to(block, mask) for mask in stage], 0)
    return block


def scatter_blocks(blocks):
    for stage in reversed(exchange_stages()):
        parts = jnp.split(blocks, len(stage) + 1, 0)
        total = parts[0].astype(F32)
        for part, mask in zip(parts[1:], stage):
            total = total + send_to(part, mask).astype(F32)
        blocks = total.astype(BF16) if blocks.shape[0] > 64 else total
    return blocks[0]


def sum_over_devices(value):
    value = jnp.full((8, 128), value)
    for stage in exchange_stages():
        value = value + sum(send_to(value, mask) for mask in stage)
    return value[0, 0]


FLAT_ROWS = sum(27 * o * i for o, i in zip(OUTPUTS, INPUTS)) // 128
STARTS = [sum(27 * o * i for o, i in zip(OUTPUTS[:k], INPUTS[:k])) // 128 for k in range(5)]
LINES = ((1, 2), (3, 4), (1, 1), (5, 4), (3, 2))


def lane_tiles(k):
    tiles = []
    for tile, (kernel, first) in enumerate(TILES):
        if kernel == k:
            tiles.append((tile, first, min(128, INPUTS[k] - first)))
    return tiles


TILES = [(k, first) for k in range(5) for first in range(0, INPUTS[k], 128)]
TILE_SCRATCH = [pltpu.VMEM((27 * OUTPUTS[k], 128), F32) for k, _ in TILES]


def weights_kernel(own, place, where_ref, blocks_ref, k1_ref, k2_ref, k3_ref, k4_ref, k5_ref, flat_ref, *tiles):
    lane = lax.broadcasted_iota(jnp.int32, (1, 128), 1)
    for device, static in enumerate(place):
        row, shift = divmod(own * device, 128)
        block = blocks_ref[where_ref[6] ^ static].astype(F32)
        if shift == 0:
            count = -(-own // 128)
            flat_ref[row : row + count, :] = block[0:count]
            continue
        count = -(-(own + shift) // 128)
        turned = pltpu.roll(block, shift, 1)
        flat_ref[row : row + 1, :] = jnp.where(lane >= shift, turned[0:1], flat_ref[row : row + 1, :])
        flat_ref[row + 1 : row + count, :] = jnp.where(lane >= shift, turned[1:count], turned[0 : count - 1])
    for k, out_ref in enumerate((k1_ref, k2_ref, k3_ref, k4_ref, k5_ref)):
        lines, group = LINES[k]
        width = INPUTS[k]
        total = 27 * OUTPUTS[k] // group
        if group == 1:
            out_ref[...] = flat_ref[STARTS[k] : STARTS[k] + total, :].astype(BF16)
            continue
        if lines == 1:
            wide = flat_ref[STARTS[k] : STARTS[k] + total, :]
        else:
            wide = jnp.concatenate([flat_ref[pl.ds(STARTS[k] + s, total, stride=lines), :] for s in range(lines)], 1)
        for tile, first, size in lane_tiles(k):
            for r in range(group):
                start = r * width + first
                tiles[tile][pl.ds(r, total, stride=group), 0:size] = wide[:, start : start + size]
            out_ref[:, first : first + size] = tiles[tile][:, 0:size].astype(BF16)


def turn_kernel(k2_ref, k3_ref, k4_ref, k5_ref, v4_ref, v3_ref, v2_ref, v1_ref):
    sources = {2: k2_ref, 3: k3_ref, 4: k4_ref, 5: k5_ref}
    for target, out_ref in ((4, v4_ref), (3, v3_ref), (2, v2_ref), (1, v1_ref)):
        lane = C + (target - 1) * G

        @pl.loop(0, 9)
        def _(part):
            start = 0
            for source in range(5, target, -1):
                outputs = OUTPUTS[source - 1]
                for c in range(3):
                    row = pl.multiple_of((part * 3 + c) * outputs, 32)
                    out_ref[part, start : start + outputs, c * G : (c + 1) * G] = sources[source][
                        pl.ds(row, outputs), lane : lane + G
                    ]
                start += outputs


def in_grid(bounds_ref, xi, extent):
    ny = SIZE_Y + 2 * extent
    y = lax.broadcasted_iota(jnp.int32, (ny, FULL[2], G), 0) + (HALO - extent)
    z = lax.broadcasted_iota(jnp.int32, (ny, FULL[2], G), 1)
    ok = (y >= bounds_ref[2]) & (y < bounds_ref[3]) & (z >= bounds_ref[4]) & (z < bounds_ref[5])
    ok = ok & (xi >= bounds_ref[0]) & (xi < bounds_ref[1])
    return jnp.where(ok, 1.0, 0.0)


def conv_plane(src_ref, weight_ref, xi, extent, depth, outputs, forward):
    ny = SIZE_Y + 2 * extent
    total = None
    for a in range(3):
        for b in range(3):
            sx, sy = (a - 1, b - 1) if forward else (1 - a, 1 - b)
            y0 = HALO - extent + sy
            window = src_ref[xi + sx, y0 : y0 + ny, :, 0:depth].reshape(ny * FULL[2], depth)
            part = a * 3 + b
            if forward:
                weight = weight_ref[part * 3 * outputs : (part + 1) * 3 * outputs, :]
                product = lax.dot_general(window, weight, NT, preferred_element_type=F32)
            else:
                product = lax.dot_general(window, weight_ref[part], NN, preferred_element_type=F32)
            total = product if total is None else total + product
    total = total.reshape(ny, FULL[2], 3 * outputs)
    first = total[:, :, 0:outputs]
    middle = total[:, :, outputs : 2 * outputs]
    last = total[:, :, 2 * outputs : 3 * outputs]
    down, up = (1, FULL[2] - 1) if forward else (FULL[2] - 1, 1)
    return middle + pltpu.roll(first, down, 1) + pltpu.roll(last, up, 1)


def forward_kernel(bounds_ref, both_ref, w1_ref, w2_ref, w3_ref, w4_ref, in_ref, own_ref):
    in_ref[:, :, :, 0:C] = both_ref[:, :, :, 0:C]
    for layer, weight_ref in enumerate((w1_ref, w2_ref, w3_ref, w4_ref)):
        extent = EXTENTS[layer]
        depth = INPUTS[layer]
        ny = SIZE_Y + 2 * extent

        @pl.loop(HALO - extent, HALO + SIZE_X + extent)
        def _(xi):
            before = conv_plane(in_ref, weight_ref, xi, extent, depth, G, True)
            slope = jnp.where(before > 0, 1.0, LEAK_SLOPE)
            growth = (before * slope * in_grid(bounds_ref, xi, extent)).astype(BF16)
            in_ref[xi, HALO - extent : HALO - extent + ny, :, depth : depth + G] = growth

    own_ref[...] = in_ref[HALO : HALO + SIZE_X, HALO : HALO + SIZE_Y, :, 2 * C : 3 * C]


def backward_kernel(
    own_size, place, bounds_ref, both_ref, in0_ref, ext_ref, w5_ref, v4_ref, v3_ref, v2_ref, v1_ref,
    refined_ref, blocks_ref, in_ref, sig_ref, turned_ref, flat_ref, *tiles,
):
    in_ref[:, :, :, 0 : 2 * C + G] = in0_ref[:, :, :, 0 : 2 * C + G]
    lo_x, lo_y = HALO - NARROW, HALO - NARROW
    nx, ny3 = SIZE_X + 2 * NARROW, SIZE_Y + 2 * NARROW
    in_ref[lo_x : lo_x + nx, lo_y : lo_y + ny3, :, 2 * C + G : 3 * C] = ext_ref[:, :, :, G : 2 * G]
    in_ref[lo_x + 1 : lo_x + nx - 1, lo_y + 1 : lo_y + ny3 - 1, :, 2 * C : 2 * C + G] = ext_ref[
        1 : nx - 1, 1 : ny3 - 1, :, 0:G
    ]
    sig_ref[:, :, :, 0:C] = both_ref[:, :, :, C : 2 * C]

    @pl.loop(0, SIZE_X)
    def _(i):
        xi = i + HALO
        last = conv_plane(in_ref, w5_ref, xi, 0, 3 * C, C, True)
        field = in_ref[xi, HALO : HALO + SIZE_Y, :, 0:C].astype(F32)
        refined_ref[i] = (field + RESIDUAL_SCALE * last).astype(BF16)

    for step, weight_ref in enumerate((v4_ref, v3_ref, v2_ref, v1_ref)):
        extent = EXTENTS[step]
        depth = INPUTS[step]
        lane = 2 * C + G - step * G
        ny = SIZE_Y + 2 * extent

        @pl.loop(HALO - extent, HALO + SIZE_X + extent)
        def _(xi):
            back = conv_plane(sig_ref, weight_ref, xi, extent, depth, G, False)
            growth = in_ref[xi, HALO - extent : HALO - extent + ny, :, lane : lane + G].astype(F32)
            slope = jnp.where(growth > 0, 1.0, LEAK_SLOPE)
            signal = (back * slope * in_grid(bounds_ref, xi, extent)).astype(BF16)
            sig_ref[xi, HALO - extent : HALO - extent + ny, :, depth : depth + G] = signal

    rows = SIZE_X * SIZE_Y * FULL[2]
    own = sig_ref[HALO : HALO + SIZE_X, HALO : HALO + SIZE_Y, :, 0 : 3 * C].astype(F32)
    z = lax.broadcasted_iota(jnp.int32, own.shape, 2)
    own = jnp.where((z >= HALO) & (z < HALO + SIZE_Z), own, 0.0).reshape(SIZE_X * SIZE_Y, FULL[2], 3 * C)
    for c in range(3):
        moved = own if c == 1 else pltpu.roll(own, FULL[2] - 1 if c == 0 else 1, 1)
        turned_ref[c * 3 * C : (c + 1) * 3 * C, :] = moved.reshape(rows, 3 * C).T.astype(BF16)
    lanes = (160, 128, 96, 64, 0)
    for a in range(3):
        for b in range(3):
            x0, y0 = HALO + a - 1, HALO + b - 1
            window = in_ref[x0 : x0 + SIZE_X, y0 : y0 + SIZE_Y, :, 0 : 3 * C].reshape(rows, 3 * C)
            product = lax.dot_general(turned_ref[...], window, NN, preferred_element_type=F32)
            for k in range(5):
                outputs = OUTPUTS[k]
                for c in range(3):
                    offset = (a * 3 + b) * 3 + c
                    start = c * 3 * C + lanes[k]
                    for tile, first, size in lane_tiles(k):
                        tiles[tile][offset * outputs : (offset + 1) * outputs, 0:size] = product[
                            start : start + outputs, first : first + size
                        ]
    flat_ref[FLAT_ROWS:, :] = jnp.zeros((flat_ref.shape[0] - FLAT_ROWS, 128), F32)
    for k in range(5):
        lines, group = LINES[k]
        width = INPUTS[k]
        total = 27 * OUTPUTS[k] // group
        if group == 1:
            flat_ref[STARTS[k] : STARTS[k] + total, :] = tiles[lane_tiles(k)[0][0]][...]
            continue
        pieces = []
        for r in range(group):
            for tile, _, size in lane_tiles(k):
                pieces.append(tiles[tile][pl.ds(r, total, stride=group), :][:, 0:size])
        wide = jnp.concatenate(pieces, 1)
        for s in range(lines):
            flat_ref[pl.ds(STARTS[k] + s, total, stride=lines), :] = wide[:, s * 128 : (s + 1) * 128]
    rows = blocks_ref.shape[1]
    lane = lax.broadcasted_iota(jnp.int32, (1, 128), 1)
    for device, static in enumerate(place):
        row, shift = divmod(own_size * device, 128)
        if shift == 0:
            block = flat_ref[row : row + rows, :]
        else:
            turned = pltpu.roll(flat_ref[row : row + rows + 1, :], 128 - shift, 1)
            block = jnp.where(lane < 128 - shift, turned[0:rows], turned[1 : rows + 1])
        blocks_ref[bounds_ref[6] ^ static] = block.astype(BF16)


def vmem(count):
    return [pl.BlockSpec(memory_space=pltpu.VMEM)] * count


def local(features, upstream, params, first_moment, second_moment):
    own = params.shape[0]
    rows = -(-own // 1024) * 8
    devices = lax.axis_size(AXES)
    nx, ny, nz = (lax.axis_size(name) for name in AXES)
    place = places(nx, ny, nz)
    bounds = []
    for axis, size in (("gx", SIZE_X), ("gy", SIZE_Y), ("gz", SIZE_Z)):
        index = lax.axis_index(axis)
        bounds.append(jnp.where(index == 0, HALO, 0))
        bounds.append(jnp.where(index == lax.axis_size(axis) - 1, HALO + size, 2 * HALO + size))
    bounds.append(place_of(*(lax.axis_index(name) for name in AXES), nx, ny, nz))
    bounds = jnp.stack(bounds).astype(jnp.int32)

    mine = jnp.pad(params, (0, rows * 128 - own)).astype(BF16).reshape(rows, 128)
    gathered = gather_blocks(mine)
    kernels = pl.pallas_call(
        functools.partial(weights_kernel, own, place),
        out_shape=tuple(jax.ShapeDtypeStruct((27 * o, i), BF16) for o, i in zip(OUTPUTS, INPUTS)),
        in_specs=[pl.BlockSpec(memory_space=pltpu.SMEM)] + vmem(1),
        out_specs=tuple(vmem(5)),
        scratch_shapes=[pltpu.VMEM((FLAT_ROWS + 2 * rows, 128), F32)]
        + TILE_SCRATCH,
        name="weights",
    )(bounds, gathered)
    turned = pl.pallas_call(
        turn_kernel,
        out_shape=tuple(jax.ShapeDtypeStruct((9, depth, 3 * G), BF16) for depth in INPUTS[:4]),
        in_specs=vmem(4),
        out_specs=tuple(vmem(4)),
        cost_estimate=pl.CostEstimate(flops=400_000_000, bytes_accessed=2_000_000, transcendentals=0),
        name="turn",
    )(*kernels[1:])

    shape = features.shape[:2] + (SIZE_Z,)
    field = features.reshape(shape + (C,))
    signal = (RESIDUAL_SCALE * upstream.reshape(shape + (C,)).astype(F32)).astype(BF16)
    both = jnp.concatenate([field, signal], 3)
    both = swap_sides(both, "gz", 2, HALO)
    both = swap_sides(both, "gx", 0, HALO)
    both = swap_sides(both, "gy", 1, HALO)

    inner, pair = pl.pallas_call(
        forward_kernel,
        out_shape=(
            jax.ShapeDtypeStruct(FULL + (3 * C,), BF16),
            jax.ShapeDtypeStruct((SIZE_X, SIZE_Y, FULL[2], C), BF16),
        ),
        in_specs=[pl.BlockSpec(memory_space=pltpu.SMEM)] + vmem(5),
        out_specs=tuple(vmem(2)),
        name="growths",
    )(bounds, both, *kernels[:4])

    pair = pair[:, :, HALO : HALO + SIZE_Z]
    pair = swap_sides(pair, "gz", 2, HALO)
    pair = swap_sides(pair, "gx", 0, NARROW)
    pair = swap_sides(pair, "gy", 1, NARROW)

    refined, blocks = pl.pallas_call(
        functools.partial(backward_kernel, own, place),
        out_shape=(
            jax.ShapeDtypeStruct((SIZE_X, SIZE_Y, FULL[2], C), BF16),
            jax.ShapeDtypeStruct((devices, rows, 128), BF16),
        ),
        in_specs=[pl.BlockSpec(memory_space=pltpu.SMEM)] + vmem(8),
        out_specs=tuple(vmem(2)),
        scratch_shapes=[
            pltpu.VMEM(FULL + (3 * C,), BF16),
            pltpu.VMEM(FULL + (3 * C,), BF16),
            pltpu.VMEM((9 * C, SIZE_X * SIZE_Y * FULL[2]), BF16),
            pltpu.VMEM((FLAT_ROWS + 2 * rows, 128), F32),
        ]
        + TILE_SCRATCH,
        name="signals",
    )(bounds, both, inner, pair, kernels[4], *turned)
    refined = refined[:, :, HALO : HALO + SIZE_Z].reshape(features.shape)

    share = scatter_blocks(blocks).reshape(-1)[:own]
    norm_sq = sum_over_devices(jnp.sum(share * share))
    factor = jnp.minimum(1.0, jnp.sqrt(own * devices / (norm_sq + NORM_EPS)))
    clipped = share * factor
    new_first = BETA_ONE * first_moment + (1.0 - BETA_ONE) * clipped
    new_second = BETA_TWO * second_moment + (1.0 - BETA_TWO) * clipped * clipped
    first_hat = new_first / (1.0 - BETA_ONE**STEP)
    second_hat = new_second / (1.0 - BETA_TWO**STEP)
    new_params = params - LEARN_RATE * first_hat / (jnp.sqrt(second_hat) + ADAM_EPS)
    return (refined, new_params, new_first, new_second)


def solution(mesh):
    return jax.shard_map(
        local,
        mesh=mesh,
        in_specs=(P("gx", "gy", "gz"),) * 2 + (P(AXES),) * 3,
        out_specs=(P("gx", "gy", "gz"),) + (P(AXES),) * 3,
        check_vma=False,
    )
```

```python
import functools

import jax
import jax.numpy as jnp
from jax import lax
from jax.experimental import pallas as pl
from jax.experimental.pallas import tpu as pltpu
from jax.sharding import PartitionSpec as P

C = 64
G = 32
STEP = 3
AXES = ("gx", "gy", "gz")

LEAK_SLOPE = 0.2
RESIDUAL_SCALE = 0.2
BETA_ONE = 0.9
BETA_TWO = 0.999
LEARN_RATE = 0.001
ADAM_EPS = 1e-08
NORM_EPS = 1e-06

SIZE_X, SIZE_Y, SIZE_Z = 4, 8, 8
HALO = 4
FULL = (SIZE_X + 2 * HALO, SIZE_Y + 2 * HALO, SIZE_Z + 2 * HALO)
EXTENTS = (3, 2, 1, 0)
PLANES = (4, 6, 4, 5)
LIMIT = pltpu.CompilerParams(vmem_limit_bytes=32 * 1024 * 1024)
NARROW = 3
INPUTS = [C + layer * G for layer in range(5)]
OUTPUTS = [G] * 4 + [C]
BF16 = jnp.bfloat16
F32 = jnp.float32
NT = (((1,), (1,)), ((), ()))
NN = (((1,), (0,)), ((), ()))


def swap_sides(cells, axis, dim, width):
    count = lax.axis_size(axis)
    size = cells.shape[dim]
    tail = lax.slice_in_dim(cells, size - width, size, axis=dim)
    head = lax.slice_in_dim(cells, 0, width, axis=dim)
    below = lax.ppermute(tail, axis, [(i, i + 1) for i in range(count - 1)])
    above = lax.ppermute(head, axis, [(i + 1, i) for i in range(count - 1)])
    return jnp.concatenate([below, cells, above], axis=dim)


def exchange_stages():
    nx, ny, nz = (lax.axis_size(name) for name in AXES)
    stages = [
        [r for r in range(1, nz)],
        [2 * r * ny * nz for r in range(1, nx // 2)],
        [ny * nz],
        [2 * r * nz for r in range(1, ny // 2)],
        [nz],
    ]
    return [stage for stage in stages if stage]


def send_to(cells, mask):
    devices = lax.axis_size(AXES)
    return lax.ppermute(cells, AXES, [(i, i ^ mask) for i in range(devices)])


def place_of(x, y, z, nx, ny, nz):
    return z + nz * ((x >> 1) + (nx // 2) * ((x & 1) + 2 * ((y >> 1) + (ny // 2) * (y & 1))))


def places(nx, ny, nz):
    return [place_of(d // (ny * nz), d // nz % ny, d % nz, nx, ny, nz) for d in range(nx * ny * nz)]


def gather_stage(block, stage):
    return jnp.concatenate([block] + [send_to(block, mask) for mask in stage], 0)


def scatter_blocks(blocks):
    stages = exchange_stages()
    for stage in reversed(stages[1:]):
        parts = jnp.split(blocks, len(stage) + 1, 0)
        total = parts[0].astype(F32)
        for part, mask in zip(parts[1:], stage):
            total = total + send_to(part, mask).astype(F32)
        blocks = total.astype(BF16) if blocks.shape[0] > 64 else total
    total = blocks.astype(F32)
    for mask in stages[0]:
        other = send_to(blocks.astype(BF16), mask).astype(F32)
        total = total + jnp.stack([other[r ^ mask] for r in range(blocks.shape[0])])
    return total


def sum_over_groups(value):
    _, ny, nz = (lax.axis_size(name) for name in AXES)
    low = [nz, ny * nz, nz + ny * nz]
    high = [stage for stage in exchange_stages()[1:] if stage[0] not in low]
    value = jnp.full((8, 128), value)
    for stage in high + [low]:
        value = value + sum(send_to(value, mask) for mask in stage)
    return value[0, 0]


FLAT_ROWS = sum(27 * o * i for o, i in zip(OUTPUTS, INPUTS)) // 128
STARTS = [sum(27 * o * i for o, i in zip(OUTPUTS[:k], INPUTS[:k])) // 128 for k in range(5)]
LINES = ((1, 2), (3, 4), (1, 1), (5, 4), (3, 2))


def lane_tiles(k):
    tiles = []
    for tile, (kernel, first) in enumerate(TILES):
        if kernel == k:
            tiles.append((tile, first, min(128, INPUTS[k] - first)))
    return tiles


TILES = [(k, first) for k in range(5) for first in range(0, INPUTS[k], 128)]
TILE_SCRATCH = [pltpu.VMEM((27 * OUTPUTS[k], 128), F32) for k, _ in TILES]


def weights_kernel(own, place, where_ref, blocks_ref, k1_ref, k2_ref, k3_ref, k4_ref, k5_ref, flat_ref, *tiles):
    lane = lax.broadcasted_iota(jnp.int32, (1, 128), 1)
    for device, static in enumerate(place):
        row, shift = divmod(own * device, 128)
        block = blocks_ref[where_ref[6] ^ static].astype(F32)
        if shift == 0:
            count = -(-own // 128)
            flat_ref[row : row + count, :] = block[0:count]
            continue
        count = -(-(own + shift) // 128)
        turned = pltpu.roll(block, shift, 1)
        flat_ref[row : row + 1, :] = jnp.where(lane >= shift, turned[0:1], flat_ref[row : row + 1, :])
        flat_ref[row + 1 : row + count, :] = jnp.where(lane >= shift, turned[1:count], turned[0 : count - 1])
    for k, out_ref in enumerate((k1_ref, k2_ref, k3_ref, k4_ref, k5_ref)):
        lines, group = LINES[k]
        width = INPUTS[k]
        total = 27 * OUTPUTS[k] // group
        if group == 1:
            out_ref[...] = flat_ref[STARTS[k] : STARTS[k] + total, :].astype(BF16)
            continue
        if lines == 1:
            wide = flat_ref[STARTS[k] : STARTS[k] + total, :]
        else:
            wide = jnp.concatenate([flat_ref[pl.ds(STARTS[k] + s, total, stride=lines), :] for s in range(lines)], 1)
        for tile, first, size in lane_tiles(k):
            for r in range(group):
                start = r * width + first
                tiles[tile][pl.ds(r, total, stride=group), 0:size] = wide[:, start : start + size]
            out_ref[:, first : first + size] = tiles[tile][:, 0:size].astype(BF16)


def turn_kernel(k2_ref, k3_ref, k4_ref, k5_ref, v4_ref, v3_ref, v2_ref, v1_ref):
    sources = {2: k2_ref, 3: k3_ref, 4: k4_ref, 5: k5_ref}
    for target, out_ref in ((4, v4_ref), (3, v3_ref), (2, v2_ref), (1, v1_ref)):
        lane = C + (target - 1) * G

        @pl.loop(0, 9, unroll=3)
        def _(part):
            start = 0
            for source in range(5, target, -1):
                outputs = OUTPUTS[source - 1]
                pieces = []
                for c in range(3):
                    row = pl.multiple_of((part * 3 + c) * outputs, 32)
                    pieces.append(sources[source][pl.ds(row, outputs), lane : lane + G])
                out_ref[part, start : start + outputs, :] = jnp.concatenate(pieces, 1)
                start += outputs


def spread_kernel(both_ref, v4_ref, out_ref):
    extent = EXTENTS[0]

    @pl.loop(HALO - extent, HALO + SIZE_X + extent, step=PLANES[extent])
    def _(xi):
        out_ref[pl.ds(xi - (HALO - extent), PLANES[extent])] = conv_plane(both_ref, v4_ref, xi, extent, C, G, False, C)


def in_grid(bounds_ref, xi, extent):
    ny = SIZE_Y + 2 * extent
    shape = (PLANES[extent], ny, FULL[2], G)
    x = lax.broadcasted_iota(jnp.int32, shape, 0) + xi
    y = lax.broadcasted_iota(jnp.int32, shape, 1) + (HALO - extent)
    z = lax.broadcasted_iota(jnp.int32, shape, 2)
    ok = (y >= bounds_ref[2]) & (y < bounds_ref[3]) & (z >= bounds_ref[4]) & (z < bounds_ref[5])
    ok = ok & (x >= bounds_ref[0]) & (x < bounds_ref[1])
    return jnp.where(ok, 1.0, 0.0)


def conv_plane(src_ref, weight_ref, xi, extent, depth, outputs, forward, lane=0):
    ny = SIZE_Y + 2 * extent
    nx = PLANES[extent]
    total = None
    for a in range(3):
        for b in range(3):
            sx, sy = (a - 1, b - 1) if forward else (1 - a, 1 - b)
            y0 = HALO - extent + sy
            window = src_ref[pl.ds(xi + sx, nx), y0 : y0 + ny, :, lane : lane + depth].reshape(nx * ny * FULL[2], depth)
            part = a * 3 + b
            if forward:
                weight = weight_ref[part * 3 * outputs : (part + 1) * 3 * outputs, :]
                product = lax.dot_general(window, weight, NT, preferred_element_type=F32)
            else:
                product = lax.dot_general(window, weight_ref[part], NN, preferred_element_type=F32)
            total = product if total is None else total + product
    total = total.reshape(nx * ny, FULL[2], 3 * outputs)
    first = total[:, :, 0:outputs]
    middle = total[:, :, outputs : 2 * outputs]
    last = total[:, :, 2 * outputs : 3 * outputs]
    down, up = (1, FULL[2] - 1) if forward else (FULL[2] - 1, 1)
    return (middle + pltpu.roll(first, down, 1) + pltpu.roll(last, up, 1)).reshape(nx, ny, FULL[2], outputs)


def forward_kernel(bounds_ref, both_ref, w1_ref, w2_ref, w3_ref, w4_ref, in_ref, own_ref):
    in_ref[:, :, :, 0:C] = both_ref[:, :, :, 0:C]
    for layer, weight_ref in enumerate((w1_ref, w2_ref, w3_ref, w4_ref)):
        extent = EXTENTS[layer]
        depth = INPUTS[layer]
        ny = SIZE_Y + 2 * extent

        @pl.loop(HALO - extent, HALO + SIZE_X + extent, step=PLANES[extent])
        def _(xi):
            before = conv_plane(in_ref, weight_ref, xi, extent, depth, G, True)
            slope = jnp.where(before > 0, 1.0, LEAK_SLOPE)
            growth = (before * slope * in_grid(bounds_ref, xi, extent)).astype(BF16)
            in_ref[pl.ds(xi, PLANES[extent]), HALO - extent : HALO - extent + ny, :, depth : depth + G] = growth

    own_ref[...] = in_ref[HALO : HALO + SIZE_X, HALO : HALO + SIZE_Y, :, 2 * C : 3 * C]


def backward_kernel(
    own_size, place, bounds_ref, both_ref, in0_ref, ext_ref, w5_ref, spread_ref, v3_ref, v2_ref, v1_ref,
    refined_ref, blocks_ref, in_ref, sig_ref, turned_ref, flat_ref, *tiles,
):
    in_ref[:, :, :, 0 : 2 * C + G] = in0_ref[:, :, :, 0 : 2 * C + G]
    lo_x, lo_y = HALO - NARROW, HALO - NARROW
    nx, ny3 = SIZE_X + 2 * NARROW, SIZE_Y + 2 * NARROW
    in_ref[lo_x : lo_x + nx, lo_y : lo_y + ny3, :, 2 * C + G : 3 * C] = ext_ref[:, :, :, G : 2 * G]
    in_ref[lo_x + 1 : lo_x + nx - 1, lo_y + 1 : lo_y + ny3 - 1, :, 2 * C : 2 * C + G] = ext_ref[
        1 : nx - 1, 1 : ny3 - 1, :, 0:G
    ]
    sig_ref[:, :, :, 0:C] = both_ref[:, :, :, C : 2 * C]

    @pl.loop(0, SIZE_X, step=PLANES[0])
    def _(i):
        xi = i + HALO
        last = conv_plane(in_ref, w5_ref, xi, 0, 3 * C, C, True)
        field = in_ref[pl.ds(xi, PLANES[0]), HALO : HALO + SIZE_Y, :, 0:C].astype(F32)
        refined_ref[pl.ds(i, PLANES[0])] = (field + RESIDUAL_SCALE * last).astype(BF16)

    for step, weight_ref in enumerate((None, v3_ref, v2_ref, v1_ref)):
        extent = EXTENTS[step]
        depth = INPUTS[step]
        lane = 2 * C + G - step * G
        ny = SIZE_Y + 2 * extent

        @pl.loop(HALO - extent, HALO + SIZE_X + extent, step=PLANES[extent])
        def _(xi):
            if weight_ref is None:
                back = spread_ref[pl.ds(xi - (HALO - extent), PLANES[extent])]
            else:
                back = conv_plane(sig_ref, weight_ref, xi, extent, depth, G, False)
            growth = in_ref[pl.ds(xi, PLANES[extent]), HALO - extent : HALO - extent + ny, :, lane : lane + G].astype(F32)
            slope = jnp.where(growth > 0, 1.0, LEAK_SLOPE)
            signal = (back * slope * in_grid(bounds_ref, xi, extent)).astype(BF16)
            sig_ref[pl.ds(xi, PLANES[extent]), HALO - extent : HALO - extent + ny, :, depth : depth + G] = signal

    rows = SIZE_X * SIZE_Y * FULL[2]
    own = sig_ref[HALO : HALO + SIZE_X, HALO : HALO + SIZE_Y, :, 0 : 3 * C].astype(F32)
    z = lax.broadcasted_iota(jnp.int32, own.shape, 2)
    own = jnp.where((z >= HALO) & (z < HALO + SIZE_Z), own, 0.0).reshape(SIZE_X * SIZE_Y, FULL[2], 3 * C)
    for c in range(3):
        moved = own if c == 1 else pltpu.roll(own, FULL[2] - 1 if c == 0 else 1, 1)
        turned_ref[c * 3 * C : (c + 1) * 3 * C, :] = moved.reshape(rows, 3 * C).T.astype(BF16)
    lanes = (160, 128, 96, 64, 0)
    for a in range(3):
        for b in range(3):
            x0, y0 = HALO + a - 1, HALO + b - 1
            window = in_ref[x0 : x0 + SIZE_X, y0 : y0 + SIZE_Y, :, 0 : 3 * C].reshape(rows, 3 * C)
            product = lax.dot_general(turned_ref[...], window, NN, preferred_element_type=F32)
            for k in range(5):
                outputs = OUTPUTS[k]
                for c in range(3):
                    offset = (a * 3 + b) * 3 + c
                    start = c * 3 * C + lanes[k]
                    for tile, first, size in lane_tiles(k):
                        tiles[tile][offset * outputs : (offset + 1) * outputs, 0:size] = product[
                            start : start + outputs, first : first + size
                        ]
    flat_ref[FLAT_ROWS:, :] = jnp.zeros((flat_ref.shape[0] - FLAT_ROWS, 128), F32)
    for k in range(5):
        lines, group = LINES[k]
        width = INPUTS[k]
        total = 27 * OUTPUTS[k] // group
        if group == 1:
            flat_ref[STARTS[k] : STARTS[k] + total, :] = tiles[lane_tiles(k)[0][0]][...]
            continue
        pieces = []
        for r in range(group):
            for tile, _, size in lane_tiles(k):
                pieces.append(tiles[tile][pl.ds(r, total, stride=group), :][:, 0:size])
        wide = jnp.concatenate(pieces, 1)
        for s in range(lines):
            flat_ref[pl.ds(STARTS[k] + s, total, stride=lines), :] = wide[:, s * 128 : (s + 1) * 128]
    rows = blocks_ref.shape[1]
    lane = lax.broadcasted_iota(jnp.int32, (1, 128), 1)
    for device, static in enumerate(place):
        row, shift = divmod(own_size * device, 128)
        if shift == 0:
            block = flat_ref[row : row + rows, :]
        else:
            turned = pltpu.roll(flat_ref[row : row + rows + 1, :], 128 - shift, 1)
            block = jnp.where(lane < 128 - shift, turned[0:rows], turned[1 : rows + 1])
        blocks_ref[bounds_ref[6] ^ static] = block.astype(BF16)


def vmem(count):
    return [pl.BlockSpec(memory_space=pltpu.VMEM)] * count


def local(features, upstream, params, first_moment, second_moment):
    own = params.shape[0]
    rows = -(-own // 1024) * 8
    devices = lax.axis_size(AXES)
    nx, ny, nz = (lax.axis_size(name) for name in AXES)
    place = places(nx, ny, nz)
    bounds = []
    for axis, size in (("gx", SIZE_X), ("gy", SIZE_Y), ("gz", SIZE_Z)):
        index = lax.axis_index(axis)
        bounds.append(jnp.where(index == 0, HALO, 0))
        bounds.append(jnp.where(index == lax.axis_size(axis) - 1, HALO + size, 2 * HALO + size))
    bounds.append(place_of(*(lax.axis_index(name) for name in AXES), nx, ny, nz))
    bounds = jnp.stack(bounds).astype(jnp.int32)

    mine = jnp.pad(params, (0, rows * 128 - own)).astype(BF16).reshape(rows, 128)
    shape = features.shape[:2] + (SIZE_Z,)
    field = features.reshape(shape + (C,))
    signal = (RESIDUAL_SCALE * upstream.reshape(shape + (C,)).astype(F32)).astype(BF16)
    both = jnp.concatenate([field, signal], 3)
    sides = [("gz", 2, HALO), ("gx", 0, HALO), ("gy", 1, HALO)]
    gathered = mine[None]
    for stage in exchange_stages():
        gathered = gather_stage(gathered, stage)
        if sides:
            both = swap_sides(both, *sides.pop(0))
            gathered, both = lax.optimization_barrier((gathered, both))
    kernels = pl.pallas_call(
        functools.partial(weights_kernel, own, place),
        out_shape=tuple(jax.ShapeDtypeStruct((27 * o, i), BF16) for o, i in zip(OUTPUTS, INPUTS)),
        in_specs=[pl.BlockSpec(memory_space=pltpu.SMEM)] + vmem(1),
        out_specs=tuple(vmem(5)),
        scratch_shapes=[pltpu.VMEM((FLAT_ROWS + 2 * rows, 128), F32)]
        + TILE_SCRATCH,
        compiler_params=LIMIT,
        name="weights",
    )(bounds, gathered)
    inner, pair = pl.pallas_call(
        forward_kernel,
        out_shape=(
            jax.ShapeDtypeStruct(FULL + (3 * C,), BF16),
            jax.ShapeDtypeStruct((SIZE_X, SIZE_Y, FULL[2], C), BF16),
        ),
        in_specs=[pl.BlockSpec(memory_space=pltpu.SMEM)] + vmem(5),
        out_specs=tuple(vmem(2)),
        compiler_params=LIMIT,
        name="growths",
    )(bounds, both, *kernels[:4])

    pair, *sources = lax.optimization_barrier((pair, *kernels[1:]))
    pair = pair[:, :, HALO : HALO + SIZE_Z]
    turned = pl.pallas_call(
        turn_kernel,
        out_shape=tuple(jax.ShapeDtypeStruct((9, depth, 3 * G), BF16) for depth in INPUTS[:4]),
        in_specs=vmem(4),
        out_specs=tuple(vmem(4)),
        cost_estimate=pl.CostEstimate(flops=400_000_000, bytes_accessed=2_000_000, transcendentals=0),
        compiler_params=LIMIT,
        name="turn",
    )(*sources)
    pair = swap_sides(pair, "gz", 2, HALO)
    pair, *turned = lax.optimization_barrier((pair, *turned))
    wide = EXTENTS[0]
    spread = pl.pallas_call(
        spread_kernel,
        out_shape=jax.ShapeDtypeStruct((SIZE_X + 2 * wide, SIZE_Y + 2 * wide, FULL[2], G), F32),
        in_specs=vmem(2),
        out_specs=vmem(1)[0],
        cost_estimate=pl.CostEstimate(flops=400_000_000, bytes_accessed=2_000_000, transcendentals=0),
        compiler_params=LIMIT,
        name="spread",
    )(both, turned[0])
    pair = swap_sides(pair, "gx", 0, NARROW)
    pair, spread = lax.optimization_barrier((pair, spread))
    pair = swap_sides(pair, "gy", 1, NARROW)

    refined, blocks = pl.pallas_call(
        functools.partial(backward_kernel, own, place),
        out_shape=(
            jax.ShapeDtypeStruct((SIZE_X, SIZE_Y, FULL[2], C), BF16),
            jax.ShapeDtypeStruct((devices, rows, 128), BF16),
        ),
        in_specs=[pl.BlockSpec(memory_space=pltpu.SMEM)] + vmem(8),
        out_specs=tuple(vmem(2)),
        scratch_shapes=[
            pltpu.VMEM(FULL + (3 * C,), BF16),
            pltpu.VMEM(FULL + (3 * C,), BF16),
            pltpu.VMEM((9 * C, SIZE_X * SIZE_Y * FULL[2]), BF16),
            pltpu.VMEM((FLAT_ROWS + 2 * rows, 128), F32),
        ]
        + TILE_SCRATCH,
        compiler_params=LIMIT,
        name="signals",
    )(bounds, both, inner, pair, kernels[4], spread, *turned[1:])
    refined = refined[:, :, HALO : HALO + SIZE_Z].reshape(features.shape)

    totals = scatter_blocks(blocks)
    share = totals[0].reshape(-1)[:own]
    entry = lax.broadcasted_iota(jnp.int32, totals.shape, 1) * 128 + lax.broadcasted_iota(jnp.int32, totals.shape, 2)
    norm_sq = sum_over_groups(jnp.sum(jnp.where(entry < own, totals * totals, 0.0)))
    factor = jnp.minimum(1.0, jnp.sqrt(own * devices / (norm_sq + NORM_EPS)))
    clipped = share * factor
    new_first = BETA_ONE * first_moment + (1.0 - BETA_ONE) * clipped
    new_second = BETA_TWO * second_moment + (1.0 - BETA_TWO) * clipped * clipped
    first_hat = new_first / (1.0 - BETA_ONE**STEP)
    second_hat = new_second / (1.0 - BETA_TWO**STEP)
    new_params = params - LEARN_RATE * first_hat / (jnp.sqrt(second_hat) + ADAM_EPS)
    return (refined, new_params, new_first, new_second)


def solution(mesh):
    return jax.shard_map(
        local,
        mesh=mesh,
        in_specs=(P("gx", "gy", "gz"),) * 2 + (P(AXES),) * 3,
        out_specs=(P("gx", "gy", "gz"),) + (P(AXES),) * 3,
        check_vma=False,
    )
```

```python
import functools

import jax
import jax.numpy as jnp
from jax import lax
from jax.experimental import pallas as pl
from jax.experimental.pallas import tpu as pltpu
from jax.sharding import PartitionSpec as P

C = 64
G = 32
STEP = 3
AXES = ("gx", "gy", "gz")

LEAK_SLOPE = 0.2
RESIDUAL_SCALE = 0.2
BETA_ONE = 0.9
BETA_TWO = 0.999
LEARN_RATE = 0.001
ADAM_EPS = 1e-08
NORM_EPS = 1e-06

SIZE_X, SIZE_Y, SIZE_Z = 4, 8, 8
HALO = 4
FULL = (SIZE_X + 2 * HALO, SIZE_Y + 2 * HALO, SIZE_Z + 2 * HALO)
EXTENTS = (3, 2, 1, 0)
PLANES = (4, 3, 4, 5)
LIMIT = pltpu.CompilerParams(vmem_limit_bytes=32 * 1024 * 1024)
NARROW = 3
INPUTS = [C + layer * G for layer in range(5)]
OUTPUTS = [G] * 4 + [C]
BF16 = jnp.bfloat16
F32 = jnp.float32
NT = (((1,), (1,)), ((), ()))
NN = (((1,), (0,)), ((), ()))


def swap_sides(cells, axis, dim, width):
    count = lax.axis_size(axis)
    size = cells.shape[dim]
    tail = lax.slice_in_dim(cells, size - width, size, axis=dim)
    head = lax.slice_in_dim(cells, 0, width, axis=dim)
    below = lax.ppermute(tail, axis, [(i, (i + 1) % count) for i in range(count)])
    above = lax.ppermute(head, axis, [((i + 1) % count, i) for i in range(count)])
    return jnp.concatenate([below, cells, above], axis=dim)


def exchange_stages():
    nx, ny, nz = (lax.axis_size(name) for name in AXES)
    stages = [
        [r for r in range(1, nz)],
        [2 * r * ny * nz for r in range(1, nx // 2)],
        [ny * nz],
        [2 * r * nz for r in range(1, ny // 2)],
        [nz],
    ]
    return [stage for stage in stages if stage]


def send_to(cells, mask):
    devices = lax.axis_size(AXES)
    return lax.ppermute(cells, AXES, [(i, i ^ mask) for i in range(devices)])


def place_of(x, y, z, nx, ny, nz):
    return z + nz * ((x >> 1) + (nx // 2) * ((x & 1) + 2 * ((y >> 1) + (ny // 2) * (y & 1))))


def places(nx, ny, nz):
    return [place_of(d // (ny * nz), d // nz % ny, d % nz, nx, ny, nz) for d in range(nx * ny * nz)]


def gather_stage(block, stage):
    return jnp.concatenate([block] + [send_to(block, mask) for mask in stage], 0)


def scatter_blocks(blocks):
    stages = exchange_stages()
    for stage in reversed(stages[1:]):
        parts = jnp.split(blocks, len(stage) + 1, 0)
        total = parts[0].astype(F32)
        for part, mask in zip(parts[1:], stage):
            total = total + send_to(part, mask).astype(F32)
        blocks = total.astype(BF16) if blocks.shape[0] > 64 else total
    total = blocks.astype(F32)
    for mask in stages[0]:
        other = send_to(blocks.astype(BF16), mask).astype(F32)
        total = total + jnp.stack([other[r ^ mask] for r in range(blocks.shape[0])])
    return total


def sum_over_groups(value):
    _, ny, nz = (lax.axis_size(name) for name in AXES)
    low = [nz, ny * nz, nz + ny * nz]
    high = [stage for stage in exchange_stages()[1:] if stage[0] not in low]
    value = jnp.full((8, 128), value)
    for stage in high + [low]:
        value = value + sum(send_to(value, mask) for mask in stage)
    return value[0, 0]


FLAT_ROWS = sum(27 * o * i for o, i in zip(OUTPUTS, INPUTS)) // 128
STARTS = [sum(27 * o * i for o, i in zip(OUTPUTS[:k], INPUTS[:k])) // 128 for k in range(5)]
LINES = ((1, 2), (3, 4), (1, 1), (5, 4), (3, 2))


def lane_tiles(k):
    tiles = []
    for tile, (kernel, first) in enumerate(TILES):
        if kernel == k:
            tiles.append((tile, first, min(128, INPUTS[k] - first)))
    return tiles


TILES = [(k, first) for k in range(5) for first in range(0, INPUTS[k], 128)]
TILE_SCRATCH = [pltpu.VMEM((27 * OUTPUTS[k], 128), F32) for k, _ in TILES]


def weights_kernel(own, place, where_ref, blocks_ref, k1_ref, k2_ref, k3_ref, k4_ref, k5_ref, flat_ref, *tiles):
    lane = lax.broadcasted_iota(jnp.int32, (1, 128), 1)
    half = len(place) // 2

    @pl.loop(0, 2)
    def _(part):
        base = pl.multiple_of(part * (own * half // 128), 8)
        me = where_ref[6] ^ (part * place[half])
        for device, static in enumerate(place[:half]):
            row, shift = divmod(own * device, 128)
            block = blocks_ref[me ^ static].astype(F32)
            if shift == 0:
                count = -(-own // 128)
                flat_ref[pl.ds(base + row, count), :] = block[0:count]
                continue
            count = -(-(own + shift) // 128)
            turned = pltpu.roll(block, shift, 1)
            first = pl.ds(base + row, 1)
            flat_ref[first, :] = jnp.where(lane >= shift, turned[0:1], flat_ref[first, :])
            flat_ref[pl.ds(base + row + 1, count - 1), :] = jnp.where(
                lane >= shift, turned[1:count], turned[0 : count - 1]
            )

    for k, out_ref in enumerate((k1_ref, k2_ref, k3_ref, k4_ref, k5_ref)):
        lines, group = LINES[k]
        width = INPUTS[k]
        total = 27 * OUTPUTS[k] // group
        if group == 1:
            out_ref[...] = flat_ref[STARTS[k] : STARTS[k] + total, :].astype(BF16)
            continue
        if lines == 1:
            wide = flat_ref[STARTS[k] : STARTS[k] + total, :]
        else:
            wide = jnp.concatenate([flat_ref[pl.ds(STARTS[k] + s, total, stride=lines), :] for s in range(lines)], 1)
        for tile, first, size in lane_tiles(k):
            for r in range(group):
                start = r * width + first
                tiles[tile][pl.ds(r, total, stride=group), 0:size] = wide[:, start : start + size]
            out_ref[:, first : first + size] = tiles[tile][:, 0:size].astype(BF16)


def turn_kernel(k2_ref, k3_ref, k4_ref, k5_ref, v4_ref, v3_ref, v2_ref, v1_ref):
    sources = {2: k2_ref, 3: k3_ref, 4: k4_ref, 5: k5_ref}
    for target, out_ref in ((4, v4_ref), (3, v3_ref), (2, v2_ref), (1, v1_ref)):
        lane = C + (target - 1) * G

        @pl.loop(0, 9)
        def _(part):
            start = 0
            for source in range(5, target, -1):
                outputs = OUTPUTS[source - 1]
                pieces = []
                for c in range(3):
                    row = pl.multiple_of((part * 3 + c) * outputs, 32)
                    pieces.append(sources[source][pl.ds(row, outputs), lane : lane + G])
                out_ref[part, start : start + outputs, :] = jnp.concatenate(pieces, 1)
                start += outputs


def spread_kernel(top_ref, v4_ref, out_ref):
    extent = EXTENTS[0]

    @pl.loop(HALO - extent, HALO + SIZE_X + extent, step=PLANES[extent])
    def _(xi):
        out_ref[pl.ds(xi - (HALO - extent), PLANES[extent])] = conv_plane(top_ref, v4_ref, xi, extent, C, G, False)


def in_grid(bounds_ref, xi, shape, y0):
    x = lax.broadcasted_iota(jnp.int32, shape, 0) + xi
    y = lax.broadcasted_iota(jnp.int32, shape, 1) + y0
    z = lax.broadcasted_iota(jnp.int32, shape, 2)
    ok = (y >= bounds_ref[2]) & (y < bounds_ref[3]) & (z >= bounds_ref[4]) & (z < bounds_ref[5])
    ok = ok & (x >= bounds_ref[0]) & (x < bounds_ref[1])
    return jnp.where(ok, 1.0, 0.0)


def conv_plane(src_ref, weight_ref, xi, extent, depth, outputs, forward):
    ny = SIZE_Y + 2 * extent
    nx = PLANES[extent]
    total = None
    for a in range(3):
        for b in range(3):
            sx, sy = (a - 1, b - 1) if forward else (1 - a, 1 - b)
            y0 = HALO - extent + sy
            window = src_ref[pl.ds(xi + sx, nx), y0 : y0 + ny, :, 0:depth].reshape(nx * ny * FULL[2], depth)
            part = a * 3 + b
            if forward:
                weight = weight_ref[part * 3 * outputs : (part + 1) * 3 * outputs, :]
                product = lax.dot_general(window, weight, NT, preferred_element_type=F32)
            else:
                product = lax.dot_general(window, weight_ref[part], NN, preferred_element_type=F32)
            total = product if total is None else total + product
    total = total.reshape(nx * ny, FULL[2], 3 * outputs)
    first = total[:, :, 0:outputs]
    middle = total[:, :, outputs : 2 * outputs]
    last = total[:, :, 2 * outputs : 3 * outputs]
    down, up = (1, FULL[2] - 1) if forward else (FULL[2] - 1, 1)
    return (middle + pltpu.roll(first, down, 1) + pltpu.roll(last, up, 1)).reshape(nx, ny, FULL[2], outputs)


def forward_kernel(bounds_ref, both_ref, w1_ref, w2_ref, w3_ref, w4_ref, in_ref, own_ref, top_ref):
    @pl.loop(0, FULL[0], step=4)
    def _(xi):
        cells = both_ref[pl.ds(xi, 4)].astype(F32)
        cells = (cells * in_grid(bounds_ref, xi, cells.shape, 0)).astype(BF16)
        in_ref[pl.ds(xi, 4), :, :, 0:C] = cells[:, :, :, 0:C]
        top_ref[pl.ds(xi, 4)] = cells[:, :, :, C : 2 * C]

    for layer, weight_ref in enumerate((w1_ref, w2_ref, w3_ref, w4_ref)):
        extent = EXTENTS[layer]
        depth = INPUTS[layer]
        ny = SIZE_Y + 2 * extent

        @pl.loop(HALO - extent, HALO + SIZE_X + extent, step=PLANES[extent])
        def _(xi):
            before = conv_plane(in_ref, weight_ref, xi, extent, depth, G, True)
            slope = jnp.where(before > 0, 1.0, LEAK_SLOPE)
            growth = (before * slope * in_grid(bounds_ref, xi, before.shape, HALO - extent)).astype(BF16)
            in_ref[pl.ds(xi, PLANES[extent]), HALO - extent : HALO - extent + ny, :, depth : depth + G] = growth

    own_ref[...] = in_ref[HALO : HALO + SIZE_X, HALO : HALO + SIZE_Y, :, 2 * C : 3 * C]


def backward_kernel(
    own_size, place, bounds_ref, top_ref, in0_ref, ext_ref, w5_ref, spread_ref, v3_ref, v2_ref, v1_ref,
    refined_ref, blocks_ref, in_ref, sig_ref, turned_ref, flat_ref, *tiles,
):
    in_ref[:, :, :, 0 : 2 * C] = in0_ref[:, :, :, 0 : 2 * C]
    sig_ref[:, :, :, 0:C] = top_ref[...]
    low, ny3 = HALO - NARROW, SIZE_Y + 2 * NARROW

    @pl.loop(0, SIZE_X + 2 * NARROW, step=5)
    def _(i):
        cells = ext_ref[pl.ds(i, 5)].astype(F32)
        cells = cells * in_grid(bounds_ref, i + low, cells.shape, low)
        in_ref[pl.ds(i + low, 5), low : low + ny3, :, 2 * C : 3 * C] = cells.astype(BF16)

    @pl.loop(0, SIZE_X, step=PLANES[0])
    def _(i):
        xi = i + HALO
        last = conv_plane(in_ref, w5_ref, xi, 0, 3 * C, C, True)
        field = in_ref[pl.ds(xi, PLANES[0]), HALO : HALO + SIZE_Y, :, 0:C].astype(F32)
        refined_ref[pl.ds(i, PLANES[0])] = (field + RESIDUAL_SCALE * last).astype(BF16)

    for step, weight_ref in enumerate((None, v3_ref, v2_ref, v1_ref)):
        extent = EXTENTS[step]
        depth = INPUTS[step]
        lane = 2 * C + G - step * G
        ny = SIZE_Y + 2 * extent

        @pl.loop(HALO - extent, HALO + SIZE_X + extent, step=PLANES[extent])
        def _(xi):
            if weight_ref is None:
                back = spread_ref[pl.ds(xi - (HALO - extent), PLANES[extent])]
            else:
                back = conv_plane(sig_ref, weight_ref, xi, extent, depth, G, False)
            growth = in_ref[pl.ds(xi, PLANES[extent]), HALO - extent : HALO - extent + ny, :, lane : lane + G].astype(F32)
            slope = jnp.where(growth > 0, 1.0, LEAK_SLOPE)
            signal = (back * slope * in_grid(bounds_ref, xi, back.shape, HALO - extent)).astype(BF16)
            sig_ref[pl.ds(xi, PLANES[extent]), HALO - extent : HALO - extent + ny, :, depth : depth + G] = signal

    rows = SIZE_X * SIZE_Y * FULL[2]
    own = sig_ref[HALO : HALO + SIZE_X, HALO : HALO + SIZE_Y, :, 0 : 3 * C].astype(F32)
    z = lax.broadcasted_iota(jnp.int32, own.shape, 2)
    own = jnp.where((z >= HALO) & (z < HALO + SIZE_Z), own, 0.0).reshape(SIZE_X * SIZE_Y, FULL[2], 3 * C)
    for c in range(3):
        moved = own if c == 1 else pltpu.roll(own, FULL[2] - 1 if c == 0 else 1, 1)
        turned_ref[c * 3 * C : (c + 1) * 3 * C, :] = moved.reshape(rows, 3 * C).T.astype(BF16)
    lanes = (160, 128, 96, 64, 0)
    for a in range(3):
        for b in range(3):
            x0, y0 = HALO + a - 1, HALO + b - 1
            window = in_ref[x0 : x0 + SIZE_X, y0 : y0 + SIZE_Y, :, 0 : 3 * C].reshape(rows, 3 * C)
            product = lax.dot_general(turned_ref[...], window, NN, preferred_element_type=F32)
            for k in range(5):
                outputs = OUTPUTS[k]
                for c in range(3):
                    offset = (a * 3 + b) * 3 + c
                    start = c * 3 * C + lanes[k]
                    for tile, first, size in lane_tiles(k):
                        tiles[tile][offset * outputs : (offset + 1) * outputs, 0:size] = product[
                            start : start + outputs, first : first + size
                        ]
    flat_ref[FLAT_ROWS:, :] = jnp.zeros((flat_ref.shape[0] - FLAT_ROWS, 128), F32)
    for k in range(5):
        lines, group = LINES[k]
        width = INPUTS[k]
        total = 27 * OUTPUTS[k] // group
        if group == 1:
            flat_ref[STARTS[k] : STARTS[k] + total, :] = tiles[lane_tiles(k)[0][0]][...]
            continue
        pieces = []
        for r in range(group):
            for tile, _, size in lane_tiles(k):
                pieces.append(tiles[tile][pl.ds(r, total, stride=group), :][:, 0:size])
        wide = jnp.concatenate(pieces, 1)
        for s in range(lines):
            flat_ref[pl.ds(STARTS[k] + s, total, stride=lines), :] = wide[:, s * 128 : (s + 1) * 128]
    rows = blocks_ref.shape[1]
    lane = lax.broadcasted_iota(jnp.int32, (1, 128), 1)
    half = len(place) // 2

    @pl.loop(0, 2)
    def _(part):
        base = pl.multiple_of(part * (own_size * half // 128), 8)
        me = bounds_ref[6] ^ (part * place[half])
        for device, static in enumerate(place[:half]):
            row, shift = divmod(own_size * device, 128)
            if shift == 0:
                block = flat_ref[pl.ds(base + row, rows), :]
            else:
                turned = pltpu.roll(flat_ref[pl.ds(base + row, rows + 1), :], 128 - shift, 1)
                block = jnp.where(lane < 128 - shift, turned[0:rows], turned[1 : rows + 1])
            blocks_ref[me ^ static] = block.astype(BF16)


def vmem(count):
    return [pl.BlockSpec(memory_space=pltpu.VMEM)] * count


def local(features, upstream, params, first_moment, second_moment):
    own = params.shape[0]
    rows = -(-own // 1024) * 8
    devices = lax.axis_size(AXES)
    nx, ny, nz = (lax.axis_size(name) for name in AXES)
    place = places(nx, ny, nz)
    bounds = []
    for axis, size in (("gx", SIZE_X), ("gy", SIZE_Y), ("gz", SIZE_Z)):
        index = lax.axis_index(axis)
        bounds.append(jnp.where(index == 0, HALO, 0))
        bounds.append(jnp.where(index == lax.axis_size(axis) - 1, HALO + size, 2 * HALO + size))
    bounds.append(place_of(*(lax.axis_index(name) for name in AXES), nx, ny, nz))
    bounds = jnp.stack(bounds).astype(jnp.int32)

    mine = jnp.pad(params, (0, rows * 128 - own)).astype(BF16).reshape(rows, 128)
    shape = features.shape[:2] + (SIZE_Z,)
    field = features.reshape(shape + (C,))
    signal = (RESIDUAL_SCALE * upstream.reshape(shape + (C,)).astype(F32)).astype(BF16)
    both = jnp.concatenate([field, signal], 3)
    sides = [("gz", 2, HALO), ("gx", 0, HALO), ("gy", 1, HALO)]
    gathered = mine[None]
    stages = exchange_stages()
    for step, stage in enumerate(stages):
        gathered = gather_stage(gathered, stage)
        side = step + len(sides) - len(stages)
        if side >= 0:
            both = swap_sides(both, *sides[side])
        gathered, both = lax.optimization_barrier((gathered, both))
    kernels = pl.pallas_call(
        functools.partial(weights_kernel, own, place),
        out_shape=tuple(jax.ShapeDtypeStruct((27 * o, i), BF16) for o, i in zip(OUTPUTS, INPUTS)),
        in_specs=[pl.BlockSpec(memory_space=pltpu.SMEM)] + vmem(1),
        out_specs=tuple(vmem(5)),
        scratch_shapes=[pltpu.VMEM((FLAT_ROWS + 2 * rows, 128), F32)]
        + TILE_SCRATCH,
        compiler_params=LIMIT,
        name="weights",
    )(bounds, gathered)
    inner, pair, top = pl.pallas_call(
        forward_kernel,
        out_shape=(
            jax.ShapeDtypeStruct(FULL + (3 * C,), BF16),
            jax.ShapeDtypeStruct((SIZE_X, SIZE_Y, FULL[2], C), BF16),
            jax.ShapeDtypeStruct(FULL + (C,), BF16),
        ),
        in_specs=[pl.BlockSpec(memory_space=pltpu.SMEM)] + vmem(5),
        out_specs=tuple(vmem(3)),
        compiler_params=LIMIT,
        name="growths",
    )(bounds, both, *kernels[:4])

    pair, *sources = lax.optimization_barrier((pair, *kernels[1:]))
    pair = pair[:, :, HALO : HALO + SIZE_Z]
    turned = pl.pallas_call(
        turn_kernel,
        out_shape=tuple(jax.ShapeDtypeStruct((9, depth, 3 * G), BF16) for depth in INPUTS[:4]),
        in_specs=vmem(4),
        out_specs=tuple(vmem(4)),
        cost_estimate=pl.CostEstimate(flops=400_000_000, bytes_accessed=2_000_000, transcendentals=0),
        compiler_params=LIMIT,
        name="turn",
    )(*sources)
    pair = swap_sides(pair, "gz", 2, HALO)
    pair, *turned = lax.optimization_barrier((pair, *turned))
    wide = EXTENTS[0]
    spread = pl.pallas_call(
        spread_kernel,
        out_shape=jax.ShapeDtypeStruct((SIZE_X + 2 * wide, SIZE_Y + 2 * wide, FULL[2], G), F32),
        in_specs=vmem(2),
        out_specs=vmem(1)[0],
        cost_estimate=pl.CostEstimate(flops=400_000_000, bytes_accessed=2_000_000, transcendentals=0),
        compiler_params=LIMIT,
        name="spread",
    )(top, turned[0])
    pair = swap_sides(pair, "gx", 0, NARROW)
    pair, spread = lax.optimization_barrier((pair, spread))
    pair = swap_sides(pair, "gy", 1, NARROW)

    refined, blocks = pl.pallas_call(
        functools.partial(backward_kernel, own, place),
        out_shape=(
            jax.ShapeDtypeStruct((SIZE_X, SIZE_Y, FULL[2], C), BF16),
            jax.ShapeDtypeStruct((devices, rows, 128), BF16),
        ),
        in_specs=[pl.BlockSpec(memory_space=pltpu.SMEM)] + vmem(8),
        out_specs=tuple(vmem(2)),
        scratch_shapes=[
            pltpu.VMEM(FULL + (3 * C,), BF16),
            pltpu.VMEM(FULL + (3 * C,), BF16),
            pltpu.VMEM((9 * C, SIZE_X * SIZE_Y * FULL[2]), BF16),
            pltpu.VMEM((FLAT_ROWS + 2 * rows, 128), F32),
        ]
        + TILE_SCRATCH,
        compiler_params=LIMIT,
        name="signals",
    )(bounds, top, inner, pair, kernels[4], spread, *turned[1:])
    refined = refined[:, :, HALO : HALO + SIZE_Z].reshape(features.shape)

    totals = scatter_blocks(blocks)
    share = totals[0].reshape(-1)[:own]
    entry = lax.broadcasted_iota(jnp.int32, totals.shape, 1) * 128 + lax.broadcasted_iota(jnp.int32, totals.shape, 2)
    norm_sq = sum_over_groups(jnp.sum(jnp.where(entry < own, totals * totals, 0.0)))
    factor = jnp.minimum(1.0, jnp.sqrt(own * devices / (norm_sq + NORM_EPS)))
    clipped = share * factor
    new_first = BETA_ONE * first_moment + (1.0 - BETA_ONE) * clipped
    new_second = BETA_TWO * second_moment + (1.0 - BETA_TWO) * clipped * clipped
    first_hat = new_first / (1.0 - BETA_ONE**STEP)
    second_hat = new_second / (1.0 - BETA_TWO**STEP)
    new_params = params - LEARN_RATE * first_hat / (jnp.sqrt(second_hat) + ADAM_EPS)
    return (refined, new_params, new_first, new_second)


def solution(mesh):
    return jax.shard_map(
        local,
        mesh=mesh,
        in_specs=(P("gx", "gy", "gz"),) * 2 + (P(AXES),) * 3,
        out_specs=(P("gx", "gy", "gz"),) + (P(AXES),) * 3,
        check_vma=False,
    )
```

```python
import functools

import jax
import jax.numpy as jnp
from jax import lax
from jax.experimental import pallas as pl
from jax.experimental.pallas import tpu as pltpu
from jax.sharding import PartitionSpec as P

C = 64
G = 32
STEP = 3
AXES = ("gx", "gy", "gz")

LEAK_SLOPE = 0.2
RESIDUAL_SCALE = 0.2
BETA_ONE = 0.9
BETA_TWO = 0.999
LEARN_RATE = 0.001
ADAM_EPS = 1e-08
NORM_EPS = 1e-06

SIZE_X, SIZE_Y, SIZE_Z = 4, 8, 8
HALO = 4
FULL = (SIZE_X + 2 * HALO, SIZE_Y + 2 * HALO, SIZE_Z + 2 * HALO)
EXTENTS = (3, 2, 1, 0)
PLANES = (4, 3, 2, 5)
SPREAD = 2
LIMIT = pltpu.CompilerParams(vmem_limit_bytes=32 * 1024 * 1024)
NARROW = 3
INPUTS = [C + layer * G for layer in range(5)]
OUTPUTS = [G] * 4 + [C]
BF16 = jnp.bfloat16
F32 = jnp.float32
NT = (((1,), (1,)), ((), ()))
NN = (((1,), (0,)), ((), ()))


def swap_sides(cells, axis, dim, width):
    count = lax.axis_size(axis)
    size = cells.shape[dim]
    tail = lax.slice_in_dim(cells, size - width, size, axis=dim)
    head = lax.slice_in_dim(cells, 0, width, axis=dim)
    below = lax.ppermute(tail, axis, [(i, (i + 1) % count) for i in range(count)])
    above = lax.ppermute(head, axis, [((i + 1) % count, i) for i in range(count)])
    return jnp.concatenate([below, cells, above], axis=dim)


def exchange_stages():
    nx, ny, nz = (lax.axis_size(name) for name in AXES)
    stages = [
        [r for r in range(1, nz)],
        [2 * r * ny * nz for r in range(1, nx // 2)],
        [ny * nz],
        [2 * r * nz for r in range(1, ny // 2)],
        [nz],
    ]
    return [stage for stage in stages if stage]


def send_to(cells, mask):
    devices = lax.axis_size(AXES)
    return lax.ppermute(cells, AXES, [(i, i ^ mask) for i in range(devices)])


def place_of(x, y, z, nx, ny, nz):
    return z + nz * ((x >> 1) + (nx // 2) * ((x & 1) + 2 * ((y >> 1) + (ny // 2) * (y & 1))))


def places(nx, ny, nz):
    return [place_of(d // (ny * nz), d // nz % ny, d % nz, nx, ny, nz) for d in range(nx * ny * nz)]


def gather_stage(block, stage):
    return [block] + [send_to(block, mask) for mask in stage]


def gather_ring(block, stage):
    half = block.shape[0] // 2
    first, last = send_to(block, stage[0]), send_to(block, stage[2])
    block, first, last = yield [block, first, last]
    low, high = send_to(last[:half], stage[0]), send_to(first[half:], stage[2])
    yield [block, first, low, high, last]


def scatter_ring(parts, stage):
    half = parts[0].shape[0] // 2
    low, high = send_to(parts[2][:half], stage[0]), send_to(parts[2][half:], stage[2])
    first = jnp.concatenate([parts[1][:half], (parts[1][half:].astype(F32) + high.astype(F32)).astype(BF16)], 0)
    last = jnp.concatenate([(parts[3][:half].astype(F32) + low.astype(F32)).astype(BF16), parts[3][half:]], 0)
    return parts[0].astype(F32) + send_to(first, stage[0]).astype(F32) + send_to(last, stage[2]).astype(F32)


def scatter_blocks(blocks):
    stages = exchange_stages()
    for stage in reversed(stages[1:]):
        parts = jnp.split(blocks, len(stage) + 1, 0)
        if len(stage) == 3 and parts[0].shape[0] >= 32:
            total = scatter_ring(parts, stage)
        else:
            total = parts[0].astype(F32)
            for part, mask in zip(parts[1:], stage):
                total = total + send_to(part, mask).astype(F32)
        blocks = total.astype(BF16) if blocks.shape[0] > 64 else total
    total = blocks.astype(F32)
    for mask in stages[0]:
        other = send_to(blocks.astype(BF16), mask).astype(F32)
        total = total + jnp.stack([other[r ^ mask] for r in range(blocks.shape[0])])
    return total


def sum_over_groups(value):
    _, ny, nz = (lax.axis_size(name) for name in AXES)
    low = [nz, ny * nz, nz + ny * nz]
    high = [stage for stage in exchange_stages()[1:] if stage[0] not in low]
    value = jnp.full((8, 128), value)
    for stage in high + [low]:
        value = value + sum(send_to(value, mask) for mask in stage)
    return value[0, 0]


FLAT_ROWS = sum(27 * o * i for o, i in zip(OUTPUTS, INPUTS)) // 128
STARTS = [sum(27 * o * i for o, i in zip(OUTPUTS[:k], INPUTS[:k])) // 128 for k in range(5)]
LINES = ((1, 2), (3, 4), (1, 1), (5, 4), (3, 2))


def lane_tiles(k):
    tiles = []
    for tile, (kernel, first) in enumerate(TILES):
        if kernel == k:
            tiles.append((tile, first, min(128, INPUTS[k] - first)))
    return tiles


TILES = [(k, first) for k in range(5) for first in range(0, INPUTS[k], 128)]
TILE_SCRATCH = [pltpu.VMEM((27 * OUTPUTS[k], 128), F32) for k, _ in TILES]


def weights_kernel(own, place, where_ref, blocks_ref, k1_ref, k2_ref, k3_ref, k4_ref, k5_ref, flat_ref, *tiles):
    lane = lax.broadcasted_iota(jnp.int32, (1, 128), 1)
    half = len(place) // 2

    @pl.loop(0, 2)
    def _(part):
        base = pl.multiple_of(part * (own * half // 128), 8)
        me = where_ref[6] ^ (part * place[half])
        for device, static in enumerate(place[:half]):
            row, shift = divmod(own * device, 128)
            block = blocks_ref[me ^ static].astype(F32)
            if shift == 0:
                count = -(-own // 128)
                flat_ref[pl.ds(base + row, count), :] = block[0:count]
                continue
            count = -(-(own + shift) // 128)
            turned = pltpu.roll(block, shift, 1)
            first = pl.ds(base + row, 1)
            flat_ref[first, :] = jnp.where(lane >= shift, turned[0:1], flat_ref[first, :])
            flat_ref[pl.ds(base + row + 1, count - 1), :] = jnp.where(
                lane >= shift, turned[1:count], turned[0 : count - 1]
            )

    for k, out_ref in enumerate((k1_ref, k2_ref, k3_ref, k4_ref, k5_ref)):
        lines, group = LINES[k]
        width = INPUTS[k]
        total = 27 * OUTPUTS[k] // group
        if group == 1:
            out_ref[...] = flat_ref[STARTS[k] : STARTS[k] + total, :].astype(BF16)
            continue
        if lines == 1:
            wide = flat_ref[STARTS[k] : STARTS[k] + total, :]
        else:
            wide = jnp.concatenate([flat_ref[pl.ds(STARTS[k] + s, total, stride=lines), :] for s in range(lines)], 1)
        for tile, first, size in lane_tiles(k):
            for r in range(group):
                start = r * width + first
                tiles[tile][pl.ds(r, total, stride=group), 0:size] = wide[:, start : start + size]
            out_ref[:, first : first + size] = tiles[tile][:, 0:size].astype(BF16)


def turn_kernel(k2_ref, k3_ref, k4_ref, k5_ref, v4_ref, v3_ref, v2_ref, v1_ref):
    sources = {2: k2_ref, 3: k3_ref, 4: k4_ref, 5: k5_ref}
    for target, out_ref in ((4, v4_ref), (3, v3_ref), (2, v2_ref), (1, v1_ref)):
        lane = C + (target - 1) * G

        @pl.loop(0, 9)
        def _(part):
            start = 0
            for source in range(5, target, -1):
                outputs = OUTPUTS[source - 1]
                pieces = []
                for c in range(3):
                    row = pl.multiple_of((part * 3 + c) * outputs, 32)
                    pieces.append(sources[source][pl.ds(row, outputs), lane : lane + G])
                out_ref[part, start : start + outputs, :] = jnp.concatenate(pieces, 1)
                start += outputs


def spread_kernel(top_ref, v4_ref, out_ref):
    extent = EXTENTS[0]

    @pl.loop(HALO - extent, HALO + SIZE_X + extent, step=SPREAD)
    def _(xi):
        out_ref[pl.ds(xi - (HALO - extent), SPREAD)] = conv_plane(top_ref, v4_ref, xi, extent, C, G, False, SPREAD)


def in_grid(bounds_ref, xi, shape, y0):
    x = lax.broadcasted_iota(jnp.int32, shape, 0) + xi
    y = lax.broadcasted_iota(jnp.int32, shape, 1) + y0
    z = lax.broadcasted_iota(jnp.int32, shape, 2)
    ok = (y >= bounds_ref[2]) & (y < bounds_ref[3]) & (z >= bounds_ref[4]) & (z < bounds_ref[5])
    ok = ok & (x >= bounds_ref[0]) & (x < bounds_ref[1])
    return jnp.where(ok, 1.0, 0.0)


def conv_plane(src_ref, weight_ref, xi, extent, depth, outputs, forward, nx):
    ny = SIZE_Y + 2 * extent
    total = None
    for a in range(3):
        for b in range(3):
            sx, sy = (a - 1, b - 1) if forward else (1 - a, 1 - b)
            y0 = HALO - extent + sy
            window = src_ref[pl.ds(xi + sx, nx), y0 : y0 + ny, :, 0:depth].reshape(nx * ny * FULL[2], depth)
            part = a * 3 + b
            if forward:
                weight = weight_ref[part * 3 * outputs : (part + 1) * 3 * outputs, :]
                product = lax.dot_general(window, weight, NT, preferred_element_type=F32)
            else:
                product = lax.dot_general(window, weight_ref[part], NN, preferred_element_type=F32)
            total = product if total is None else total + product
    total = total.reshape(nx * ny, FULL[2], 3 * outputs)
    first = total[:, :, 0:outputs]
    middle = total[:, :, outputs : 2 * outputs]
    last = total[:, :, 2 * outputs : 3 * outputs]
    down, up = (1, FULL[2] - 1) if forward else (FULL[2] - 1, 1)
    return (middle + pltpu.roll(first, down, 1) + pltpu.roll(last, up, 1)).reshape(nx, ny, FULL[2], outputs)


def forward_kernel(bounds_ref, both_ref, w1_ref, w2_ref, w3_ref, w4_ref, in_ref, own_ref, top_ref):
    @pl.loop(0, FULL[0], step=4)
    def _(xi):
        cells = both_ref[pl.ds(xi, 4)].astype(F32)
        cells = (cells * in_grid(bounds_ref, xi, cells.shape, 0)).astype(BF16)
        in_ref[pl.ds(xi, 4), :, :, 0:C] = cells[:, :, :, 0:C]
        top_ref[pl.ds(xi, 4)] = cells[:, :, :, C : 2 * C]

    for layer, weight_ref in enumerate((w1_ref, w2_ref, w3_ref, w4_ref)):
        extent = EXTENTS[layer]
        depth = INPUTS[layer]
        ny = SIZE_Y + 2 * extent

        @pl.loop(HALO - extent, HALO + SIZE_X + extent, step=PLANES[extent])
        def _(xi):
            before = conv_plane(in_ref, weight_ref, xi, extent, depth, G, True, PLANES[extent])
            slope = jnp.where(before > 0, 1.0, LEAK_SLOPE)
            growth = (before * slope * in_grid(bounds_ref, xi, before.shape, HALO - extent)).astype(BF16)
            in_ref[pl.ds(xi, PLANES[extent]), HALO - extent : HALO - extent + ny, :, depth : depth + G] = growth

    own_ref[...] = in_ref[HALO : HALO + SIZE_X, HALO : HALO + SIZE_Y, :, 2 * C : 3 * C]


def backward_kernel(
    own_size, place, bounds_ref, top_ref, in0_ref, ext_ref, spread_ref, v3_ref, v2_ref, v1_ref,
    in_ref, blocks_ref, sig_ref, turned_ref, flat_ref, *tiles,
):
    in_ref[:, :, :, 0 : 2 * C] = in0_ref[:, :, :, 0 : 2 * C]
    sig_ref[:, :, :, 0:C] = top_ref[...]
    low, ny3 = HALO - NARROW, SIZE_Y + 2 * NARROW

    @pl.loop(0, SIZE_X + 2 * NARROW, step=5)
    def _(i):
        cells = ext_ref[pl.ds(i, 5)].astype(F32)
        cells = cells * in_grid(bounds_ref, i + low, cells.shape, low)
        in_ref[pl.ds(i + low, 5), low : low + ny3, :, 2 * C : 3 * C] = cells.astype(BF16)

    for step, weight_ref in enumerate((None, v3_ref, v2_ref, v1_ref)):
        extent = EXTENTS[step]
        depth = INPUTS[step]
        lane = 2 * C + G - step * G
        ny = SIZE_Y + 2 * extent

        @pl.loop(HALO - extent, HALO + SIZE_X + extent, step=PLANES[extent])
        def _(xi):
            if weight_ref is None:
                back = spread_ref[pl.ds(xi - (HALO - extent), PLANES[extent])]
            else:
                back = conv_plane(sig_ref, weight_ref, xi, extent, depth, G, False, PLANES[extent])
            growth = in_ref[pl.ds(xi, PLANES[extent]), HALO - extent : HALO - extent + ny, :, lane : lane + G].astype(F32)
            slope = jnp.where(growth > 0, 1.0, LEAK_SLOPE)
            signal = (back * slope * in_grid(bounds_ref, xi, back.shape, HALO - extent)).astype(BF16)
            sig_ref[pl.ds(xi, PLANES[extent]), HALO - extent : HALO - extent + ny, :, depth : depth + G] = signal

    rows = SIZE_X * SIZE_Y * FULL[2]
    own = sig_ref[HALO : HALO + SIZE_X, HALO : HALO + SIZE_Y, :, 0 : 3 * C].astype(F32)
    z = lax.broadcasted_iota(jnp.int32, own.shape, 2)
    own = jnp.where((z >= HALO) & (z < HALO + SIZE_Z), own, 0.0).reshape(SIZE_X * SIZE_Y, FULL[2], 3 * C)
    for c in range(3):
        moved = own if c == 1 else pltpu.roll(own, FULL[2] - 1 if c == 0 else 1, 1)
        turned_ref[c * 3 * C : (c + 1) * 3 * C, :] = moved.reshape(rows, 3 * C).T.astype(BF16)
    lanes = (160, 128, 96, 64, 0)
    for a in range(3):
        for b in range(3):
            x0, y0 = HALO + a - 1, HALO + b - 1
            window = in_ref[x0 : x0 + SIZE_X, y0 : y0 + SIZE_Y, :, 0 : 3 * C].reshape(rows, 3 * C)
            product = lax.dot_general(turned_ref[...], window, NN, preferred_element_type=F32)
            for k in range(5):
                outputs = OUTPUTS[k]
                for c in range(3):
                    offset = (a * 3 + b) * 3 + c
                    start = c * 3 * C + lanes[k]
                    for tile, first, size in lane_tiles(k):
                        tiles[tile][offset * outputs : (offset + 1) * outputs, 0:size] = product[
                            start : start + outputs, first : first + size
                        ]
    flat_ref[FLAT_ROWS:, :] = jnp.zeros((flat_ref.shape[0] - FLAT_ROWS, 128), F32)
    for k in range(5):
        lines, group = LINES[k]
        width = INPUTS[k]
        total = 27 * OUTPUTS[k] // group
        if group == 1:
            flat_ref[STARTS[k] : STARTS[k] + total, :] = tiles[lane_tiles(k)[0][0]][...]
            continue
        pieces = []
        for r in range(group):
            for tile, _, size in lane_tiles(k):
                pieces.append(tiles[tile][pl.ds(r, total, stride=group), :][:, 0:size])
        wide = jnp.concatenate(pieces, 1)
        for s in range(lines):
            flat_ref[pl.ds(STARTS[k] + s, total, stride=lines), :] = wide[:, s * 128 : (s + 1) * 128]
    rows = blocks_ref.shape[1]
    lane = lax.broadcasted_iota(jnp.int32, (1, 128), 1)
    half = len(place) // 2

    @pl.loop(0, 2)
    def _(part):
        base = pl.multiple_of(part * (own_size * half // 128), 8)
        me = bounds_ref[6] ^ (part * place[half])
        for device, static in enumerate(place[:half]):
            row, shift = divmod(own_size * device, 128)
            if shift == 0:
                block = flat_ref[pl.ds(base + row, rows), :]
            else:
                turned = pltpu.roll(flat_ref[pl.ds(base + row, rows + 1), :], 128 - shift, 1)
                block = jnp.where(lane < 128 - shift, turned[0:rows], turned[1 : rows + 1])
            blocks_ref[me ^ static] = block.astype(BF16)


def refine_kernel(in_ref, w5_ref, refined_ref):
    @pl.loop(0, SIZE_X, step=2)
    def _(i):
        xi = i + HALO
        last = conv_plane(in_ref, w5_ref, xi, 0, 3 * C, C, True, 2)
        field = in_ref[pl.ds(xi, 2), HALO : HALO + SIZE_Y, :, 0:C].astype(F32)
        refined_ref[pl.ds(i, 2)] = (field + RESIDUAL_SCALE * last).astype(BF16)


def vmem(count):
    return [pl.BlockSpec(memory_space=pltpu.VMEM)] * count


def local(features, upstream, params, first_moment, second_moment):
    own = params.shape[0]
    rows = -(-own // 1024) * 8
    devices = lax.axis_size(AXES)
    nx, ny, nz = (lax.axis_size(name) for name in AXES)
    place = places(nx, ny, nz)
    bounds = []
    for axis, size in (("gx", SIZE_X), ("gy", SIZE_Y), ("gz", SIZE_Z)):
        index = lax.axis_index(axis)
        bounds.append(jnp.where(index == 0, HALO, 0))
        bounds.append(jnp.where(index == lax.axis_size(axis) - 1, HALO + size, 2 * HALO + size))
    bounds.append(place_of(*(lax.axis_index(name) for name in AXES), nx, ny, nz))
    bounds = jnp.stack(bounds).astype(jnp.int32)

    mine = jnp.pad(params, (0, rows * 128 - own)).astype(BF16).reshape(rows, 128)
    shape = features.shape[:2] + (SIZE_Z,)
    field = features.reshape(shape + (C,))
    signal = (RESIDUAL_SCALE * upstream.reshape(shape + (C,)).astype(F32)).astype(BF16)
    both = jnp.concatenate([field, signal], 3)
    sides = [("gz", 2, HALO), ("gx", 0, HALO), ("gy", 1, HALO)]
    gathered = mine[None]
    for stage in exchange_stages():
        ring = len(stage) == 3 and gathered.shape[0] >= 32
        if ring:
            steps = gather_ring(gathered, stage)
            pieces = next(steps)
        else:
            pieces = gather_stage(gathered, stage)
        if sides and (gathered.shape[0] >= 16 or len(exchange_stages()) < 5):
            both = swap_sides(both, *sides.pop(0))
        *pieces, both = lax.optimization_barrier((*pieces, both))
        if ring:
            pieces = steps.send(pieces)
            both = swap_sides(both, *sides.pop(0))
            *pieces, both = lax.optimization_barrier((*pieces, both))
        gathered = jnp.concatenate(pieces, 0)
    kernels = pl.pallas_call(
        functools.partial(weights_kernel, own, place),
        out_shape=tuple(jax.ShapeDtypeStruct((27 * o, i), BF16) for o, i in zip(OUTPUTS, INPUTS)),
        in_specs=[pl.BlockSpec(memory_space=pltpu.SMEM)] + vmem(1),
        out_specs=tuple(vmem(5)),
        scratch_shapes=[pltpu.VMEM((FLAT_ROWS + 2 * rows, 128), F32)]
        + TILE_SCRATCH,
        compiler_params=LIMIT,
        name="weights",
    )(bounds, gathered)
    inner, pair, top = pl.pallas_call(
        forward_kernel,
        out_shape=(
            jax.ShapeDtypeStruct(FULL + (3 * C,), BF16),
            jax.ShapeDtypeStruct((SIZE_X, SIZE_Y, FULL[2], C), BF16),
            jax.ShapeDtypeStruct(FULL + (C,), BF16),
        ),
        in_specs=[pl.BlockSpec(memory_space=pltpu.SMEM)] + vmem(5),
        out_specs=tuple(vmem(3)),
        compiler_params=LIMIT,
        name="growths",
    )(bounds, both, *kernels[:4])

    pair, *sources = lax.optimization_barrier((pair, *kernels[1:]))
    pair = pair[:, :, HALO : HALO + SIZE_Z]
    turned = pl.pallas_call(
        turn_kernel,
        out_shape=tuple(jax.ShapeDtypeStruct((9, depth, 3 * G), BF16) for depth in INPUTS[:4]),
        in_specs=vmem(4),
        out_specs=tuple(vmem(4)),
        cost_estimate=pl.CostEstimate(flops=400_000_000, bytes_accessed=2_000_000, transcendentals=0),
        compiler_params=LIMIT,
        name="turn",
    )(*sources)
    pair = swap_sides(pair, "gz", 2, HALO)
    pair, *turned = lax.optimization_barrier((pair, *turned))
    wide = EXTENTS[0]
    spread = pl.pallas_call(
        spread_kernel,
        out_shape=jax.ShapeDtypeStruct((SIZE_X + 2 * wide, SIZE_Y + 2 * wide, FULL[2], G), F32),
        in_specs=vmem(2),
        out_specs=vmem(1)[0],
        cost_estimate=pl.CostEstimate(flops=400_000_000, bytes_accessed=2_000_000, transcendentals=0),
        compiler_params=LIMIT,
        name="spread",
    )(top, turned[0])
    pair = swap_sides(pair, "gx", 0, NARROW)
    pair, spread = lax.optimization_barrier((pair, spread))
    pair = swap_sides(pair, "gy", 1, NARROW)

    inner, blocks = pl.pallas_call(
        functools.partial(backward_kernel, own, place),
        out_shape=(
            jax.ShapeDtypeStruct(FULL + (3 * C,), BF16),
            jax.ShapeDtypeStruct((devices, rows, 128), BF16),
        ),
        in_specs=[pl.BlockSpec(memory_space=pltpu.SMEM)] + vmem(7),
        out_specs=tuple(vmem(2)),
        scratch_shapes=[
            pltpu.VMEM(FULL + (3 * C,), BF16),
            pltpu.VMEM((9 * C, SIZE_X * SIZE_Y * FULL[2]), BF16),
            pltpu.VMEM((FLAT_ROWS + 2 * rows, 128), F32),
        ]
        + TILE_SCRATCH,
        compiler_params=LIMIT,
        name="signals",
    )(bounds, top, inner, pair, spread, *turned[1:])
    refined = pl.pallas_call(
        refine_kernel,
        out_shape=jax.ShapeDtypeStruct((SIZE_X, SIZE_Y, FULL[2], C), BF16),
        in_specs=vmem(2),
        out_specs=vmem(1)[0],
        cost_estimate=pl.CostEstimate(flops=400_000_000, bytes_accessed=2_000_000, transcendentals=0),
        compiler_params=LIMIT,
        name="refine",
    )(inner, kernels[4])
    refined = refined[:, :, HALO : HALO + SIZE_Z].reshape(features.shape)

    totals = scatter_blocks(blocks)
    share = totals[0].reshape(-1)[:own]
    entry = lax.broadcasted_iota(jnp.int32, totals.shape, 1) * 128 + lax.broadcasted_iota(jnp.int32, totals.shape, 2)
    norm_sq = sum_over_groups(jnp.sum(jnp.where(entry < own, totals * totals, 0.0)))
    factor = jnp.minimum(1.0, jnp.sqrt(own * devices / (norm_sq + NORM_EPS)))
    clipped = share * factor
    new_first = BETA_ONE * first_moment + (1.0 - BETA_ONE) * clipped
    new_second = BETA_TWO * second_moment + (1.0 - BETA_TWO) * clipped * clipped
    first_hat = new_first / (1.0 - BETA_ONE**STEP)
    second_hat = new_second / (1.0 - BETA_TWO**STEP)
    new_params = params - LEARN_RATE * first_hat / (jnp.sqrt(second_hat) + ADAM_EPS)
    return (refined, new_params, new_first, new_second)


def solution(mesh):
    return jax.shard_map(
        local,
        mesh=mesh,
        in_specs=(P("gx", "gy", "gz"),) * 2 + (P(AXES),) * 3,
        out_specs=(P("gx", "gy", "gz"),) + (P(AXES),) * 3,
        check_vma=False,
    )
```
